32 devices in a mesh: dp: 8 (over z, y), section: 4 (over x, core).
Axes of the slice: x: 2, y: 2, z: 4, core: 2. Of those that a mesh axis runs over, the one named last changes fastest.
Arguments:
- slot_of_token: int32 [2, 1, 1024], P(None, None, 'dp'), may hold values from -1 to 127, as said below
- gate_prob: float32 [2, 1, 1024], P(None, None, 'dp'), may hold values from 0.2 to 1
- layer_input: bfloat16 [1, 1024, 7168], P(None, 'dp', 'section'), may hold values from -6 to 6
- preact: bfloat16 [1, 1024, 2048], P(None, 'dp', 'section'), may hold values from -6 to 6
- top_grad: bfloat16 [1, 1024, 3584], P(None, 'dp'), may hold values from -6 to 6
- w_up: bfloat16 [1024, 7168], P('dp', 'section'), may hold values from -0.09375 to 0.09375
- w_down: bfloat16 [1024, 7168], P('dp', 'section'), may hold values from -0.1875 to 0.1875
Outputs:
- grad_inputs: bfloat16 [1, 1024, 7168], P(None, 'dp', 'section')
- grad_up: float32 [1024, 7168], P('dp', 'section')
- grad_down: float32 [1024, 7168], P('dp', 'section')
The draws below stay inside these ranges and needn't reach their ends.
Inputs may be any that keep to these rules, and one draw needn't show every extreme that they name: `slot_of_token`: within one layer, one micro-batch and the 128 tokens of one data replica, the values other than -1 are distinct; -1 marks a token that is not routed to the expert or dropped.
All inputs are finite; a program needn't handle non-finite values.
Results may differ from the reference program's by a relative error of at most 0.0098.
Values may be sent and summed in bfloat16 or wider, within the bound.
A program may use at most 128 MiB of HBM per device.

```python
import jax
import jax.numpy as jnp

D = 3584
F = 1024
SLOTS = 128
MB = 1
TOK = 128
LAYERS = 2
TOKENS = 1024
N_DP = 8


def draw_slot_of_token(key, part):
    blocks = LAYERS * MB * (TOKENS // TOK)
    block_keys = jax.random.split(key, blocks)

    def draw_block(block_key):
        shuffle_key, drop_key = jax.random.split(block_key)
        shuffled = jax.random.permutation(shuffle_key, SLOTS)[:TOK]
        kept_mask = jax.random.randint(drop_key, (TOK,), 0, 8) > 0
        return jnp.where(kept_mask, shuffled, -1).astype(jnp.int32)
    return jax.vmap(draw_block)(block_keys).reshape(LAYERS, MB, TOKENS)


def block_scale(rng, extent, cuts, low, largest):
    def one(axis_at, shards_of):
        heights = jax.random.uniform(jax.random.fold_in(jax.random.fold_in(rng, 6), axis_at), (shards_of,), jnp.float32, low / len(cuts), largest / len(cuts))
        return jnp.repeat(jnp.exp(heights), extent[axis_at] // shards_of).reshape((-1,) + (1,) * (len(extent) - axis_at - 1))

    factor_of = one(*cuts[0])
    for cut in cuts[1:]:
        factor_of = factor_of * one(*cut)
    return factor_of


def bell_draw(rng, shape, scale, bound, cuts=(), held_as=jnp.bfloat16):
    values = scale * jax.random.normal(rng, shape, jnp.float32)
    if cuts:
        values = values * block_scale(rng, shape, cuts, -0.22, 0.18)
    return jnp.clip(values, -bound, bound).astype(held_as)


def setup_inputs(seed: int = 0) -> dict:
    arg_keys = jax.random.split(jax.random.key(seed), 8)
    slot_of_token = draw_slot_of_token(jax.random.fold_in(arg_keys[7], 71), 0)
    gate_prob = jnp.clip(0.2 + 0.8 * jax.random.uniform(arg_keys[1], (LAYERS, MB, TOKENS), jnp.float32) ** block_scale(arg_keys[1], (LAYERS, MB, TOKENS), ((2, 8),), -0.2, 0.2), 0.2, 1.0)
    layer_input = bell_draw(arg_keys[2], (MB, TOKENS, LAYERS * D), 1.0, 6.0, ((1, 8), (2, 4)))
    preact = bell_draw(arg_keys[3], (MB, SLOTS * N_DP, LAYERS * F), 1.5, 6.0, ((1, 8), (2, 4)))
    top_grad = bell_draw(arg_keys[4], (MB, TOKENS, D), 1.0, 6.0, ((1, 8),))
    w_up = bell_draw(arg_keys[5], (F, LAYERS * D), D ** -0.5, 0.09375, ((0, 8), (1, 4)))
    w_down = bell_draw(arg_keys[6], (F, LAYERS * D), F ** -0.5, 0.1875, ((0, 8), (1, 4)))
    return dict(slot_of_token=slot_of_token, gate_prob=gate_prob, layer_input=layer_input, preact=preact, top_grad=top_grad, w_up=w_up, w_down=w_down)


def silu_slope(pre):
    sigmoid_val = jax.nn.sigmoid(pre)
    return sigmoid_val * (1.0 + pre * (1.0 - sigmoid_val))


def reference(slot_of_token, gate_prob, layer_input, preact, top_grad, w_up, w_down):
    groups = TOKENS // TOK
    grad_now = top_grad.reshape(MB, groups, TOK, D)
    slot_ids = jnp.arange(SLOTS, dtype=jnp.int32)
    inputs_out = []
    up_out = []
    down_out = []
    for layer in reversed(range(LAYERS)):
        slots_here = slot_of_token[layer].reshape(MB, groups, TOK)
        gates_here = gate_prob[layer].reshape(MB, groups, TOK)
        onehot = (slots_here[:, :, None, :] == slot_ids[None, None, :, None]).astype(jnp.float32)
        inputs_here = layer_input[:, :, layer * D:(layer + 1) * D].reshape(MB, groups, TOK, D)
        pre_here = preact[:, :, layer * F:(layer + 1) * F].reshape(MB * groups * SLOTS, F).astype(jnp.float32)
        up_here = w_up[:, layer * D:(layer + 1) * D]
        down_here = w_down[:, layer * D:(layer + 1) * D]
        scaled = (gates_here[..., None] * grad_now.astype(jnp.float32)).astype(jnp.bfloat16)
        slot_grad = jnp.einsum('mgst,mgtd->mgsd', onehot, scaled.astype(jnp.float32)).astype(jnp.bfloat16).reshape(-1, D)
        slot_inputs = jnp.einsum('mgst,mgtd->mgsd', onehot, inputs_here.astype(jnp.float32)).astype(jnp.bfloat16).reshape(-1, D)
        hidden_grad = jnp.dot(slot_grad, down_here.T, preferred_element_type=jnp.float32)
        pre_grad = (hidden_grad * silu_slope(pre_here)).astype(jnp.bfloat16)
        hidden = jax.nn.silu(pre_here).astype(jnp.bfloat16)
        slot_input_grad = jnp.dot(pre_grad, up_here, preferred_element_type=jnp.float32).astype(jnp.bfloat16)
        slot_input_grad = slot_input_grad.reshape(MB, groups, SLOTS, D)
        delta = jnp.einsum('mgst,mgsd->mgtd', onehot, slot_input_grad.astype(jnp.float32))
        grad_now = (grad_now.astype(jnp.float32) + delta).astype(jnp.bfloat16)
        inputs_out.append(grad_now.reshape(MB, TOKENS, D))
        up_out.append(jnp.dot(pre_grad.T, slot_inputs, preferred_element_type=jnp.float32))
        down_out.append(jnp.dot(hidden.T, slot_grad, preferred_element_type=jnp.float32))
    grad_inputs = jnp.concatenate(inputs_out[::-1], axis=2)
    grad_up = jnp.concatenate(up_out[::-1], axis=1)
    grad_down = jnp.concatenate(down_out[::-1], axis=1)
    return (grad_inputs, grad_up, grad_down)
```

```python
import functools

import jax
import jax.numpy as jnp
from jax import lax
from jax.experimental import pallas as pl
from jax.experimental.pallas import tpu as pltpu
from jax.sharding import PartitionSpec as P

MESH = pl.DeviceIdType.MESH
BF16 = jnp.bfloat16
F32 = jnp.float32
NT = (((1,), (1,)), ((), ()))
TN = (((0,), (0,)), ((), ()))


def silu_slope(pre):
    sigmoid_val = jax.nn.sigmoid(pre)
    return sigmoid_val * (1.0 + pre * (1.0 - sigmoid_val))


class Gather:
    def __init__(self, buf, push_sem, fwd_sem, recv_sem, me, n):
        self.buf, self.push_sem, self.fwd_sem, self.recv_sem = buf, push_sem, fwd_sem, recv_sem
        self.me, self.n, self.half = me, n, n // 2
        self.mate = me + 1 - 2 * lax.rem(me, 2)

    def copy(self, block, to, sem):
        return pltpu.make_async_remote_copy(
            src_ref=self.buf.at[block], dst_ref=self.buf.at[block], send_sem=sem,
            recv_sem=self.recv_sem.at[block], device_id={"dp": to}, device_id_type=MESH,
        )

    def row(self, k):
        return lax.rem(self.me - 2 * k + 2 * self.n, self.n)

    def other(self, k):
        return lax.rem(self.mate - 2 * k + 2 * self.n, self.n)

    def push_copy(self, k):
        return self.copy(self.me, lax.rem(self.me + 2 * k, self.n), self.push_sem.at[k])

    def mate_copy(self):
        return self.copy(self.me, self.mate, self.push_sem.at[0])

    def fwd_copy(self, k):
        return self.copy(self.row(k), self.mate, self.fwd_sem.at[k])

    def push(self):
        self.mate_copy().start()

        @pl.loop(1, self.half)
        def _(k):
            self.push_copy(k).start()

    def wait_block(self, block):
        self.copy(block, self.mate, self.fwd_sem.at[0]).wait_recv()

    def forward(self):
        @pl.loop(1, self.half)
        def _(k):
            self.wait_block(self.row(k))
            self.fwd_copy(k).start()

    def drain(self):
        self.mate_copy().wait_send()

        @pl.loop(1, self.half)
        def _(k):
            self.push_copy(k).wait_send()
            self.fwd_copy(k).wait_send()


def kernel(
    n, layers, slot_row, slot_col, gate_col, x_ref, pre_ref, top_ref, up_ref, down_ref,
    gin_ref, gup_ref, gdown_ref,
    sg_all, up_all, xs_all, pre_all, slope_all, hid_all, part_mine, part_other, pg_all, pg_own, acc, inc,
    sg_push, sg_fwd, sg_recv, up_push, up_fwd, up_recv, xs_push, xs_fwd, xs_recv,
    pre_send, pre_recv, pre_mate_send, pre_mate_recv, part_send, part_recv, pg_send, pg_recv,
    down_send, down_recv,
):
    me = lax.axis_index("dp")
    sec = lax.axis_index("section")
    pair, core = sec // 2, lax.rem(sec, 2)
    twin = sec + 1 - 2 * core
    half_n = n // 2
    slots, half = x_ref.shape
    is_first = pair == layers - 1

    sg = Gather(sg_all, sg_push, sg_fwd, sg_recv, me, n)
    up = Gather(up_all, up_push, up_fwd, up_recv, me, n)
    xs = Gather(xs_all, xs_push, xs_fwd, xs_recv, me, n)

    barrier = pltpu.get_barrier_semaphore()

    @pl.loop(1, n)
    def _(k):
        pl.semaphore_signal(barrier, inc=1, device_id={"dp": lax.rem(me + k, n)}, device_id_type=MESH)

    pl.semaphore_signal(barrier, inc=1, device_id={"section": twin}, device_id_type=MESH)

    @pl.when(pair > 0)
    def _():
        pl.semaphore_signal(barrier, inc=1, device_id={"section": sec - 2}, device_id_type=MESH)

    @pl.when(pair < layers - 1)
    def _():
        pl.semaphore_signal(barrier, inc=1, device_id={"section": sec + 2}, device_id_type=MESH)

    onehot = (slot_row[...] == lax.broadcasted_iota(jnp.int32, (slots, slots), 0)).astype(BF16)

    def make_slot_grad():
        scaled = (gate_col[...] * inc[...].astype(F32)).astype(BF16)
        sg_all[me] = jnp.dot(onehot, scaled, preferred_element_type=F32).astype(BF16)

    @pl.when(is_first)
    def _():
        inc[...] = top_ref[:, pl.ds(pl.multiple_of(core * half, 128), half)]
        make_slot_grad()

    up_all[me] = up_ref[...]
    xs_all[me] = jnp.dot(onehot, x_ref[...], preferred_element_type=F32).astype(BF16)

    near_pairs = (pair > 0).astype(jnp.int32) + (pair < layers - 1).astype(jnp.int32)
    pl.semaphore_wait(barrier, n + near_pairs)

    @pl.when(is_first)
    def _():
        sg.push()

    owner_core = me // half_n

    def pre_copy(j):
        to = core * half_n + j
        return pltpu.make_async_remote_copy(
            src_ref=pre_ref.at[j], dst_ref=pre_all.at[me], send_sem=pre_send.at[j],
            recv_sem=pre_recv.at[me], device_id={"dp": to}, device_id_type=MESH,
        )

    def pre_mate_copy():
        return pltpu.make_async_remote_copy(
            src_ref=pre_all, dst_ref=pre_all, send_sem=pre_mate_send.at[0],
            recv_sem=pre_mate_recv.at[0], device_id={"section": twin}, device_id_type=MESH,
        )

    @pl.when(owner_core == core)
    def _():
        pre_all[me] = pre_ref[me - core * half_n]

    @pl.loop(0, half_n)
    def _(j):
        @pl.when(core * half_n + j != me)
        def _():
            pre_copy(j).start()

    up.push()

    def take_pre():
        @pl.when(owner_core == core)
        def _():
            @pl.loop(1, n)
            def _(k):
                src = lax.rem(me + k, n)
                pltpu.make_async_remote_copy(
                    src_ref=pre_ref.at[0], dst_ref=pre_all.at[src], send_sem=pre_send.at[0],
                    recv_sem=pre_recv.at[src], device_id={"dp": src}, device_id_type=MESH,
                ).wait_recv()

            pre_mate_copy().start()

        @pl.when(owner_core != core)
        def _():
            pre_mate_copy().wait_recv()

        @pl.loop(0, n)
        def _(b):
            pre = pre_all[b].astype(F32)
            slope_all[b] = silu_slope(pre)
            hid_all[b] = jax.nn.silu(pre).astype(BF16)

    def down_copy():
        return pltpu.make_async_remote_copy(
            src_ref=gin_ref, dst_ref=inc, send_sem=down_send.at[0],
            recv_sem=down_recv.at[0], device_id={"section": sec - 2}, device_id_type=MESH,
        )

    @pl.when(jnp.logical_not(is_first))
    def _():
        xs.push()
        take_pre()
        up.forward()
        xs.forward()
        pltpu.make_async_remote_copy(
            src_ref=gin_ref, dst_ref=inc, send_sem=down_send.at[0],
            recv_sem=down_recv.at[0], device_id={"section": sec + 2}, device_id_type=MESH,
        ).wait_recv()
        make_slot_grad()
        sg.push()

    def part_copy(b):
        return pltpu.make_async_remote_copy(
            src_ref=part_mine.at[b], dst_ref=part_other.at[b], send_sem=part_send.at[b],
            recv_sem=part_recv.at[b], device_id={"section": twin}, device_id_type=MESH,
        )

    def part_of(b):
        part_mine[b] = lax.dot_general(sg_all[b], down_ref[...], NT, preferred_element_type=F32)
        part_copy(b).start()

    def pg_copy(b):
        return pltpu.make_async_remote_copy(
            src_ref=pg_all.at[b], dst_ref=pg_own.at[me], send_sem=pg_send.at[b],
            recv_sem=pg_recv.at[me], device_id={"dp": b}, device_id_type=MESH,
        )

    def finish_of(b):
        part_copy(b).wait_recv()
        pg_all[b] = ((part_mine[b] + part_other[b]) * slope_all[b]).astype(BF16)

        @pl.when(b == me)
        def _():
            pg_own[me] = pg_all[me]

        @pl.when(b != me)
        def _():
            pg_copy(b).start()

    part_of(me)

    @pl.loop(1, half_n)
    def _(k):
        sg.wait_block(sg.row(k))
        sg.fwd_copy(k).start()
        part_of(sg.row(k))

    @pl.when(is_first)
    def _():
        take_pre()

    @pl.loop(0, half_n)
    def _(k):
        finish_of(sg.row(k))

    @pl.loop(0, half_n)
    def _(k):
        sg.wait_block(sg.other(k))
        part_of(sg.other(k))
        finish_of(sg.other(k))

    @pl.when(is_first)
    def _():
        up.forward()
        xs.push()

    def wait_pg(b):
        pltpu.make_async_remote_copy(
            src_ref=pg_all.at[b], dst_ref=pg_own.at[b], send_sem=pg_send.at[b],
            recv_sem=pg_recv.at[b], device_id={"dp": b}, device_id_type=MESH,
        ).wait_recv()

    acc[...] = jnp.dot(pg_own[me], up_all[me], preferred_element_type=F32)

    @pl.loop(1, half_n)
    def _(k):
        b = up.row(k)
        wait_pg(b)
        acc[...] += jnp.dot(pg_own[b], up_all[b], preferred_element_type=F32)

    @pl.loop(0, half_n)
    def _(k):
        b = up.other(k)
        up.wait_block(b)
        wait_pg(b)
        acc[...] += jnp.dot(pg_own[b], up_all[b], preferred_element_type=F32)

    onehot_t = (slot_col[...] == lax.broadcasted_iota(jnp.int32, (slots, slots), 1)).astype(BF16)
    delta = jnp.dot(onehot_t, acc[...].astype(BF16), preferred_element_type=F32)
    gin_ref[...] = (inc[...].astype(F32) + delta).astype(BF16)

    @pl.when(pair > 0)
    def _():
        down_copy().start()

    @pl.when(is_first)
    def _():
        xs.forward()

    def weight_grad(out_ref, left, right):
        out_ref[...] = lax.dot_general(left[0], right[0], TN, preferred_element_type=F32)

        @pl.loop(1, n)
        def _(b):
            out_ref[...] += lax.dot_general(left[b], right[b], TN, preferred_element_type=F32)

    weight_grad(gdown_ref, hid_all, sg_all)

    @pl.loop(0, half_n)
    def _(k):
        xs.wait_block(xs.other(k))

    weight_grad(gup_ref, pg_all, xs_all)

    sg.drain()
    up.drain()
    xs.drain()

    @pl.loop(0, half_n)
    def _(j):
        @pl.when(core * half_n + j != me)
        def _():
            pre_copy(j).wait_send()

    @pl.when(owner_core == core)
    def _():
        pre_mate_copy().wait_send()

    @pl.loop(0, n)
    def _(b):
        part_copy(b).wait_send()

        @pl.when(b != me)
        def _():
            pg_copy(b).wait_send()

    @pl.when(pair > 0)
    def _():
        down_copy().wait_send()


def local(n, layers, slot_of_token, gate_prob, layer_input, preact, top_grad, w_up, w_down):
    pair = lax.axis_index("section") // 2
    slots, half = layer_input.shape[1:]
    units = w_up.shape[0]
    slot_here = lax.dynamic_index_in_dim(slot_of_token, pair, 0, keepdims=False)
    gate_here = lax.dynamic_index_in_dim(gate_prob, pair, 0, keepdims=False)
    pre = preact[0].reshape(slots, n // 2, units).transpose(1, 0, 2)
    vmem = pl.BlockSpec(memory_space=pltpu.VMEM)
    dma = lambda count: pltpu.SemaphoreType.DMA((count,))
    wide = pltpu.VMEM((n, slots, half), BF16)
    thin = lambda dtype: pltpu.VMEM((n, slots, units), dtype)
    gin, gup, gdown = pl.pallas_call(
        functools.partial(kernel, n, layers),
        out_shape=[
            jax.ShapeDtypeStruct((slots, half), BF16),
            jax.ShapeDtypeStruct((units, half), F32),
            jax.ShapeDtypeStruct((units, half), F32),
        ],
        in_specs=[vmem] * 8,
        out_specs=[vmem] * 3,
        scratch_shapes=[
            wide, pltpu.VMEM((n, units, half), BF16), wide,
            thin(BF16), thin(F32), thin(BF16), thin(F32), thin(F32), thin(BF16), thin(BF16),
            pltpu.VMEM((slots, half), F32),
            pltpu.VMEM((slots, half), BF16),
            dma(n // 2), dma(n // 2), dma(n), dma(n // 2), dma(n // 2), dma(n), dma(n // 2), dma(n // 2), dma(n),
            dma(n // 2), dma(n), dma(1), dma(1), dma(n), dma(n), dma(n), dma(n),
            dma(1), dma(1),
        ],
        compiler_params=pltpu.CompilerParams(
            collective_id=0, has_side_effects=True, vmem_limit_bytes=62 * 1024 * 1024
        ),
    )(
        slot_here, slot_here.reshape(slots, 1), gate_here.reshape(slots, 1),
        layer_input[0], pre, top_grad[0], w_up, w_down,
    )
    return gin[None], gup, gdown


def solution(mesh):
    n, sections = mesh.shape["dp"], mesh.shape["section"]
    in_specs = (
        P(None, None, "dp"),
        P(None, None, "dp"),
        P(None, "dp", "section"),
        P(None, "dp", "section"),
        P(None, "dp", None),
        P("dp", "section"),
        P("dp", "section"),
    )
    out_specs = (P(None, "dp", "section"), P("dp", "section"), P("dp", "section"))
    return jax.shard_map(
        functools.partial(local, n, sections // 2), mesh=mesh, in_specs=in_specs, out_specs=out_specs, check_vma=False
    )
```

```python
import functools

import jax
import jax.numpy as jnp
from jax import lax
from jax.experimental import pallas as pl
from jax.experimental.pallas import tpu as pltpu
from jax.sharding import PartitionSpec as P

MESH = pl.DeviceIdType.MESH
BF16 = jnp.bfloat16
F32 = jnp.float32
NT = (((1,), (1,)), ((), ()))
TN = (((0,), (0,)), ((), ()))


def silu_slope(pre):
    sigmoid_val = jax.nn.sigmoid(pre)
    return sigmoid_val * (1.0 + pre * (1.0 - sigmoid_val))


class Gather:
    def __init__(self, buf, right_sem, left_sem, mate_sem, recv_sem, me, n):
        self.buf, self.recv_sem = buf, recv_sem
        self.right_sem, self.left_sem, self.mate_sem = right_sem, left_sem, mate_sem
        self.me, self.last, self.at, self.side = me, n // 2 - 1, me // 2, lax.rem(me, 2)
        self.mate = me + 1 - 2 * self.side

    def copy(self, block, to, sem):
        return pltpu.make_async_remote_copy(
            src_ref=self.buf.at[block], dst_ref=self.buf.at[block], send_sem=sem,
            recv_sem=self.recv_sem.at[block], device_id={"dp": to}, device_id_type=MESH,
        )

    def row(self, i):
        return 2 * i + self.side

    def other(self, i):
        return 2 * i + 1 - self.side

    def right(self, i):
        return self.copy(self.row(i), self.me + 2, self.right_sem.at[i])

    def left(self, i):
        return self.copy(self.row(i), self.me - 2, self.left_sem.at[i])

    def to_mate(self, i):
        return self.copy(self.row(i), self.mate, self.mate_sem.at[i])

    def go_right(self, i):
        @pl.when(self.at < self.last)
        def _():
            self.right(i).start()

    def go_left(self, i):
        @pl.when(self.at > 0)
        def _():
            self.left(i).start()

    def begin(self):
        self.go_right(self.at)
        self.go_left(self.at)
        self.to_mate(self.at).start()

    def wait_block(self, block):
        self.copy(block, self.mate, self.mate_sem.at[0]).wait_recv()

    def walk(self, visit_low, visit_high):
        @pl.loop(1, self.last + 1)
        def _(j):
            @pl.when(self.at - j >= 0)
            def _():
                visit_low(self.at - j)

            @pl.when(self.at + j <= self.last)
            def _():
                visit_high(self.at + j)

    def relay(self, use=lambda block: None):
        def low(i):
            self.wait_block(self.row(i))
            self.go_right(i)
            self.to_mate(i).start()
            use(self.row(i))

        def high(i):
            self.wait_block(self.row(i))
            self.go_left(i)
            self.to_mate(i).start()
            use(self.row(i))

        self.walk(low, high)

    def each_row(self, use):
        self.walk(lambda i: use(self.row(i)), lambda i: use(self.row(i)))

    def each_other(self, use):
        def visit(i):
            self.wait_block(self.other(i))
            use(self.other(i))

        visit(self.at)
        self.walk(visit, visit)

    def drain(self):
        @pl.loop(0, self.last + 1)
        def _(i):
            self.to_mate(i).wait_send()

            @pl.when(jnp.logical_and(self.at < self.last, i <= self.at))
            def _():
                self.right(i).wait_send()

            @pl.when(jnp.logical_and(self.at > 0, i >= self.at))
            def _():
                self.left(i).wait_send()


def kernel(
    n, layers, slot_row, slot_col, gate_col, x_ref, pre_ref, top_ref, up_ref, down_ref,
    gin_ref, gup_ref, gdown_ref,
    sg_all, up_all, xs_all, pre_all, slope_all, hid_all, part_mine, part_other, pg_all, pg_own, acc, inc,
    sg_right, sg_left, sg_mate, sg_recv, up_right, up_left, up_mate, up_recv, xs_right, xs_left, xs_mate, xs_recv,
    pre_send, pre_recv, pre_mate_send, pre_mate_recv, part_send, part_recv, pg_send, pg_recv,
    down_send, down_recv,
):
    me = lax.axis_index("dp")
    sec = lax.axis_index("section")
    pair, core = sec // 2, lax.rem(sec, 2)
    twin = sec + 1 - 2 * core
    half_n = n // 2
    slots, half = x_ref.shape
    is_first = pair == layers - 1

    sg = Gather(sg_all, sg_right, sg_left, sg_mate, sg_recv, me, n)
    up = Gather(up_all, up_right, up_left, up_mate, up_recv, me, n)
    xs = Gather(xs_all, xs_right, xs_left, xs_mate, xs_recv, me, n)

    barrier = pltpu.get_barrier_semaphore()

    @pl.loop(1, n)
    def _(k):
        pl.semaphore_signal(barrier, inc=1, device_id={"dp": lax.rem(me + k, n)}, device_id_type=MESH)

    pl.semaphore_signal(barrier, inc=1, device_id={"section": twin}, device_id_type=MESH)

    @pl.when(pair > 0)
    def _():
        pl.semaphore_signal(barrier, inc=1, device_id={"section": sec - 2}, device_id_type=MESH)

    @pl.when(pair < layers - 1)
    def _():
        pl.semaphore_signal(barrier, inc=1, device_id={"section": sec + 2}, device_id_type=MESH)

    onehot = (slot_row[...] == lax.broadcasted_iota(jnp.int32, (slots, slots), 0)).astype(BF16)

    def make_slot_grad():
        scaled = (gate_col[...] * inc[...].astype(F32)).astype(BF16)
        sg_all[me] = jnp.dot(onehot, scaled, preferred_element_type=F32).astype(BF16)

    @pl.when(is_first)
    def _():
        inc[...] = top_ref[:, pl.ds(pl.multiple_of(core * half, 128), half)]
        make_slot_grad()

    up_all[me] = up_ref[...]

    near_pairs = (pair > 0).astype(jnp.int32) + (pair < layers - 1).astype(jnp.int32)
    pl.semaphore_wait(barrier, n + near_pairs)

    @pl.when(is_first)
    def _():
        sg.begin()

    @pl.when(jnp.logical_not(is_first))
    def _():
        up.begin()

    owner_core = me // half_n

    def pre_copy(j):
        to = core * half_n + j
        return pltpu.make_async_remote_copy(
            src_ref=pre_ref.at[j], dst_ref=pre_all.at[me], send_sem=pre_send.at[j],
            recv_sem=pre_recv.at[me], device_id={"dp": to}, device_id_type=MESH,
        )

    def pre_mate_copy():
        return pltpu.make_async_remote_copy(
            src_ref=pre_all, dst_ref=pre_all, send_sem=pre_mate_send.at[0],
            recv_sem=pre_mate_recv.at[0], device_id={"section": twin}, device_id_type=MESH,
        )

    @pl.when(owner_core == core)
    def _():
        pre_all[me] = pre_ref[me - core * half_n]

    @pl.loop(0, half_n)
    def _(j):
        @pl.when(core * half_n + j != me)
        def _():
            pre_copy(j).start()

    xs_all[me] = jnp.dot(onehot, x_ref[...], preferred_element_type=F32).astype(BF16)
    gup_ref[...] = jnp.zeros_like(gup_ref)
    gdown_ref[...] = jnp.zeros_like(gdown_ref)

    def take_pre():
        @pl.when(owner_core == core)
        def _():
            @pl.loop(1, n)
            def _(k):
                src = lax.rem(me + k, n)
                pltpu.make_async_remote_copy(
                    src_ref=pre_ref.at[0], dst_ref=pre_all.at[src], send_sem=pre_send.at[0],
                    recv_sem=pre_recv.at[src], device_id={"dp": src}, device_id_type=MESH,
                ).wait_recv()

            pre_mate_copy().start()

        @pl.when(owner_core != core)
        def _():
            pre_mate_copy().wait_recv()

        @pl.loop(0, n)
        def _(b):
            pre = pre_all[b].astype(F32)
            slope_all[b] = silu_slope(pre)
            hid_all[b] = jax.nn.silu(pre).astype(BF16)

    def down_copy():
        return pltpu.make_async_remote_copy(
            src_ref=gin_ref, dst_ref=inc, send_sem=down_send.at[0],
            recv_sem=down_recv.at[0], device_id={"section": sec - 2}, device_id_type=MESH,
        )

    @pl.when(jnp.logical_not(is_first))
    def _():
        take_pre()
        up.relay()
        xs.begin()
        xs.relay()
        pltpu.make_async_remote_copy(
            src_ref=gin_ref, dst_ref=inc, send_sem=down_send.at[0],
            recv_sem=down_recv.at[0], device_id={"section": sec + 2}, device_id_type=MESH,
        ).wait_recv()
        make_slot_grad()
        sg.begin()

    def part_copy(b):
        return pltpu.make_async_remote_copy(
            src_ref=part_mine.at[b], dst_ref=part_other.at[b], send_sem=part_send.at[b],
            recv_sem=part_recv.at[b], device_id={"section": twin}, device_id_type=MESH,
        )

    def part_of(b):
        part_mine[b] = lax.dot_general(sg_all[b], down_ref[...], NT, preferred_element_type=F32)
        part_copy(b).start()

    def pg_copy(b):
        return pltpu.make_async_remote_copy(
            src_ref=pg_all.at[b], dst_ref=pg_own.at[me], send_sem=pg_send.at[b],
            recv_sem=pg_recv.at[me], device_id={"dp": b}, device_id_type=MESH,
        )

    def finish_of(b):
        part_copy(b).wait_recv()
        pg_all[b] = ((part_mine[b] + part_other[b]) * slope_all[b]).astype(BF16)

        @pl.when(b == me)
        def _():
            pg_own[me] = pg_all[me]

        @pl.when(b != me)
        def _():
            pg_copy(b).start()

    def add_down(b):
        gdown_ref[...] += lax.dot_general(hid_all[b], sg_all[b], TN, preferred_element_type=F32)

    def add_up(b):
        gup_ref[...] += lax.dot_general(pg_all[b], xs_all[b], TN, preferred_element_type=F32)

    def finish_row(b):
        finish_of(b)
        add_down(b)

        @pl.when(jnp.logical_not(is_first))
        def _():
            add_up(b)

    def finish_other(b):
        part_of(b)
        add_down(b)
        finish_of(b)

        @pl.when(jnp.logical_not(is_first))
        def _():
            xs.wait_block(b)
            add_up(b)

    part_of(me)
    sg.relay(part_of)

    @pl.when(is_first)
    def _():
        up.begin()
        take_pre()

    finish_row(me)
    sg.each_row(finish_row)
    sg.each_other(finish_other)

    @pl.when(is_first)
    def _():
        up.relay()
        xs.begin()

    def wait_pg(b):
        pltpu.make_async_remote_copy(
            src_ref=pg_all.at[b], dst_ref=pg_own.at[b], send_sem=pg_send.at[b],
            recv_sem=pg_recv.at[b], device_id={"dp": b}, device_id_type=MESH,
        ).wait_recv()

    acc[...] = jnp.dot(pg_own[me], up_all[me], preferred_element_type=F32)

    def add_acc(b):
        wait_pg(b)
        acc[...] += jnp.dot(pg_own[b], up_all[b], preferred_element_type=F32)

    up.each_row(add_acc)
    up.each_other(add_acc)

    onehot_t = (slot_col[...] == lax.broadcasted_iota(jnp.int32, (slots, slots), 1)).astype(BF16)
    delta = jnp.dot(onehot_t, acc[...].astype(BF16), preferred_element_type=F32)
    gin_ref[...] = (inc[...].astype(F32) + delta).astype(BF16)

    @pl.when(pair > 0)
    def _():
        down_copy().start()

    @pl.when(is_first)
    def _():
        xs.relay()
        add_up(me)
        xs.each_row(add_up)
        xs.each_other(add_up)

    sg.drain()
    up.drain()
    xs.drain()

    @pl.loop(0, half_n)
    def _(j):
        @pl.when(core * half_n + j != me)
        def _():
            pre_copy(j).wait_send()

    @pl.when(owner_core == core)
    def _():
        pre_mate_copy().wait_send()

    @pl.loop(0, n)
    def _(b):
        part_copy(b).wait_send()

        @pl.when(b != me)
        def _():
            pg_copy(b).wait_send()

    @pl.when(pair > 0)
    def _():
        down_copy().wait_send()


def local(n, layers, slot_of_token, gate_prob, layer_input, preact, top_grad, w_up, w_down):
    pair = lax.axis_index("section") // 2
    slots, half = layer_input.shape[1:]
    units = w_up.shape[0]
    slot_here = lax.dynamic_index_in_dim(slot_of_token, pair, 0, keepdims=False)
    gate_here = lax.dynamic_index_in_dim(gate_prob, pair, 0, keepdims=False)
    pre = preact[0].reshape(slots, n // 2, units).transpose(1, 0, 2)
    vmem = pl.BlockSpec(memory_space=pltpu.VMEM)
    dma = lambda count: pltpu.SemaphoreType.DMA((count,))
    wide = pltpu.VMEM((n, slots, half), BF16)
    thin = lambda dtype: pltpu.VMEM((n, slots, units), dtype)
    gin, gup, gdown = pl.pallas_call(
        functools.partial(kernel, n, layers),
        out_shape=[
            jax.ShapeDtypeStruct((slots, half), BF16),
            jax.ShapeDtypeStruct((units, half), F32),
            jax.ShapeDtypeStruct((units, half), F32),
        ],
        in_specs=[vmem] * 8,
        out_specs=[vmem] * 3,
        scratch_shapes=[
            wide, pltpu.VMEM((n, units, half), BF16), wide,
            thin(BF16), thin(F32), thin(BF16), thin(F32), thin(F32), thin(BF16), thin(BF16),
            pltpu.VMEM((slots, half), F32),
            pltpu.VMEM((slots, half), BF16),
            *([dma(n // 2), dma(n // 2), dma(n // 2), dma(n)] * 3),
            dma(n // 2), dma(n), dma(1), dma(1), dma(n), dma(n), dma(n), dma(n),
            dma(1), dma(1),
        ],
        compiler_params=pltpu.CompilerParams(
            collective_id=0, has_side_effects=True, vmem_limit_bytes=62 * 1024 * 1024
        ),
    )(
        slot_here, slot_here.reshape(slots, 1), gate_here.reshape(slots, 1),
        layer_input[0], pre, top_grad[0], w_up, w_down,
    )
    return gin[None], gup, gdown


def solution(mesh):
    n, sections = mesh.shape["dp"], mesh.shape["section"]
    in_specs = (
        P(None, None, "dp"),
        P(None, None, "dp"),
        P(None, "dp", "section"),
        P(None, "dp", "section"),
        P(None, "dp", None),
        P("dp", "section"),
        P("dp", "section"),
    )
    out_specs = (P(None, "dp", "section"), P("dp", "section"), P("dp", "section"))
    return jax.shard_map(
        functools.partial(local, n, sections // 2), mesh=mesh, in_specs=in_specs, out_specs=out_specs, check_vma=False
    )
```

```python
import functools

import jax
import jax.numpy as jnp
from jax import lax
from jax.experimental import pallas as pl
from jax.experimental.pallas import tpu as pltpu
from jax.sharding import PartitionSpec as P

MESH = pl.DeviceIdType.MESH
BF16 = jnp.bfloat16
F32 = jnp.float32
NT = (((1,), (1,)), ((), ()))
TN = (((0,), (0,)), ((), ()))


def silu_slope(pre):
    sigmoid_val = jax.nn.sigmoid(pre)
    return sigmoid_val * (1.0 + pre * (1.0 - sigmoid_val))


class Gather:
    def __init__(self, buf, right_sem, left_sem, mate_sem, recv_sem, me, n):
        self.buf, self.recv_sem = buf, recv_sem
        self.right_sem, self.left_sem, self.mate_sem = right_sem, left_sem, mate_sem
        self.me, self.last, self.at, self.side = me, n // 2 - 1, me // 2, lax.rem(me, 2)
        self.mate = me + 1 - 2 * self.side

    def copy(self, block, to, sem):
        return pltpu.make_async_remote_copy(
            src_ref=self.buf.at[block], dst_ref=self.buf.at[block], send_sem=sem,
            recv_sem=self.recv_sem.at[block], device_id={"dp": to}, device_id_type=MESH,
        )

    def row(self, i):
        return 2 * i + self.side

    def other(self, i):
        return 2 * i + 1 - self.side

    def right(self, i):
        return self.copy(self.row(i), self.me + 2, self.right_sem.at[i])

    def left(self, i):
        return self.copy(self.row(i), self.me - 2, self.left_sem.at[i])

    def to_mate(self, i):
        return self.copy(self.row(i), self.mate, self.mate_sem.at[i])

    def go_right(self, i):
        @pl.when(self.at < self.last)
        def _():
            self.right(i).start()

    def go_left(self, i):
        @pl.when(self.at > 0)
        def _():
            self.left(i).start()

    def begin(self):
        self.go_right(self.at)
        self.go_left(self.at)
        self.to_mate(self.at).start()

    def wait_block(self, block):
        self.copy(block, self.mate, self.mate_sem.at[0]).wait_recv()

    def walk(self, visit_low, visit_high):
        @pl.loop(1, self.last + 1)
        def _(j):
            @pl.when(self.at - j >= 0)
            def _():
                visit_low(self.at - j)

            @pl.when(self.at + j <= self.last)
            def _():
                visit_high(self.at + j)

    def relay(self, use=lambda block: None, forward=True):
        def low(i):
            self.wait_block(self.row(i))
            self.go_right(i)
            if forward:
                self.to_mate(i).start()
            use(self.row(i))

        def high(i):
            self.wait_block(self.row(i))
            self.go_left(i)
            if forward:
                self.to_mate(i).start()
            use(self.row(i))

        self.walk(low, high)

    def each_row(self, use):
        self.walk(lambda i: use(self.row(i)), lambda i: use(self.row(i)))

    def each_other(self, use):
        def visit(i):
            self.wait_block(self.other(i))
            use(self.other(i))

        visit(self.at)
        self.walk(visit, visit)

    def drain(self):
        @pl.loop(0, self.last + 1)
        def _(i):
            self.to_mate(i).wait_send()

            @pl.when(jnp.logical_and(self.at < self.last, i <= self.at))
            def _():
                self.right(i).wait_send()

            @pl.when(jnp.logical_and(self.at > 0, i >= self.at))
            def _():
                self.left(i).wait_send()


def kernel(
    n, layers, slot_row, slot_col, gate_col, x_ref, pre_ref, top_ref, up_ref, down_ref,
    gin_ref, gup_ref, gdown_ref,
    sg_all, up_all, xs_all, pre_all, slope_all, hid_all, part_mine, part_other, pg_all, pg_own, acc, inc,
    down_mate, pre_m, part2_mine, part2_other, pg_m,
    sg_right, sg_left, sg_mate, sg_recv, up_right, up_left, up_mate, up_recv, xs_right, xs_left, xs_mate, xs_recv,
    pre_send, pre_recv, pre_mate_send, pre_mate_recv, part_send, part_recv, pg_send, pg_recv,
    down_send, down_recv, dm_send, dm_recv, pm_send, pm_recv, p2_send, p2_recv, pgx_send, pgx_recv, pg2_send,
):
    me = lax.axis_index("dp")
    sec = lax.axis_index("section")
    pair, core = sec // 2, lax.rem(sec, 2)
    twin = sec + 1 - 2 * core
    half_n = n // 2
    slots, half = x_ref.shape
    is_first = pair == layers - 1

    sg = Gather(sg_all, sg_right, sg_left, sg_mate, sg_recv, me, n)
    up = Gather(up_all, up_right, up_left, up_mate, up_recv, me, n)
    xs = Gather(xs_all, xs_right, xs_left, xs_mate, xs_recv, me, n)

    barrier = pltpu.get_barrier_semaphore()

    @pl.loop(1, n)
    def _(k):
        pl.semaphore_signal(barrier, inc=1, device_id={"dp": lax.rem(me + k, n)}, device_id_type=MESH)

    pl.semaphore_signal(barrier, inc=1, device_id={"section": twin}, device_id_type=MESH)

    @pl.when(pair > 0)
    def _():
        pl.semaphore_signal(barrier, inc=1, device_id={"section": sec - 2}, device_id_type=MESH)

    @pl.when(pair < layers - 1)
    def _():
        pl.semaphore_signal(barrier, inc=1, device_id={"section": sec + 2}, device_id_type=MESH)

    onehot = (slot_row[...] == lax.broadcasted_iota(jnp.int32, (slots, slots), 0)).astype(BF16)

    def make_slot_grad():
        scaled = (gate_col[...] * inc[...].astype(F32)).astype(BF16)
        sg_all[me] = jnp.dot(onehot, scaled, preferred_element_type=F32).astype(BF16)

    @pl.when(is_first)
    def _():
        inc[...] = top_ref[:, pl.ds(pl.multiple_of(core * half, 128), half)]
        make_slot_grad()

    up_all[me] = up_ref[...]

    near_pairs = (pair > 0).astype(jnp.int32) + (pair < layers - 1).astype(jnp.int32)
    pl.semaphore_wait(barrier, n + near_pairs)

    mate = sg.mate

    def dm_copy():
        return pltpu.make_async_remote_copy(
            src_ref=down_ref, dst_ref=down_mate, send_sem=dm_send.at[0],
            recv_sem=dm_recv.at[0], device_id={"dp": mate}, device_id_type=MESH,
        )

    def pm_copy(i):
        return pltpu.make_async_remote_copy(
            src_ref=pre_all.at[sg.other(i)], dst_ref=pre_m.at[i], send_sem=pm_send.at[i],
            recv_sem=pm_recv.at[i], device_id={"dp": mate}, device_id_type=MESH,
        )

    def p2_copy(i):
        return pltpu.make_async_remote_copy(
            src_ref=part2_mine.at[i], dst_ref=part2_other.at[i], send_sem=p2_send.at[i],
            recv_sem=p2_recv.at[i], device_id={"section": twin}, device_id_type=MESH,
        )

    def pgx_copy(i, block):
        return pltpu.make_async_remote_copy(
            src_ref=pg_m.at[i], dst_ref=pg_all.at[block], send_sem=pgx_send.at[i],
            recv_sem=pgx_recv.at[i], device_id={"dp": mate}, device_id_type=MESH,
        )

    def pg2_copy(i):
        return pltpu.make_async_remote_copy(
            src_ref=pg_m.at[i], dst_ref=pg_own.at[mate], send_sem=pg2_send.at[i],
            recv_sem=pg_recv.at[mate], device_id={"dp": sg.row(i)}, device_id_type=MESH,
        )

    def part2_of(i):
        part2_mine[i] = lax.dot_general(sg_all[sg.row(i)], down_mate[...], NT, preferred_element_type=F32)
        p2_copy(i).start()

    def finish2(i):
        p2_copy(i).wait_recv()
        pm_copy(i).wait_recv()
        slope = silu_slope(pre_m[i].astype(F32))
        pg_m[i] = ((part2_mine[i] + part2_other[i]) * slope).astype(BF16)
        pgx_copy(i, sg.row(i)).start()

        @pl.when(i == sg.at)
        def _():
            pg_own[mate] = pg_m[i]

        @pl.when(i != sg.at)
        def _():
            pg2_copy(i).start()

    @pl.when(is_first)
    def _():
        dm_copy().start()
        sg.begin()

    @pl.when(jnp.logical_not(is_first))
    def _():
        up.begin()

    owner_core = me // half_n

    def pre_copy(j):
        to = core * half_n + j
        return pltpu.make_async_remote_copy(
            src_ref=pre_ref.at[j], dst_ref=pre_all.at[me], send_sem=pre_send.at[j],
            recv_sem=pre_recv.at[me], device_id={"dp": to}, device_id_type=MESH,
        )

    def pre_mate_copy():
        return pltpu.make_async_remote_copy(
            src_ref=pre_all, dst_ref=pre_all, send_sem=pre_mate_send.at[0],
            recv_sem=pre_mate_recv.at[0], device_id={"section": twin}, device_id_type=MESH,
        )

    @pl.when(owner_core == core)
    def _():
        pre_all[me] = pre_ref[me - core * half_n]

    @pl.loop(0, half_n)
    def _(j):
        @pl.when(core * half_n + j != me)
        def _():
            pre_copy(j).start()

    xs_all[me] = jnp.dot(onehot, x_ref[...], preferred_element_type=F32).astype(BF16)
    gup_ref[...] = jnp.zeros_like(gup_ref)
    gdown_ref[...] = jnp.zeros_like(gdown_ref)

    def take_pre():
        @pl.when(owner_core == core)
        def _():
            @pl.loop(1, n)
            def _(k):
                src = lax.rem(me + k, n)
                pltpu.make_async_remote_copy(
                    src_ref=pre_ref.at[0], dst_ref=pre_all.at[src], send_sem=pre_send.at[0],
                    recv_sem=pre_recv.at[src], device_id={"dp": src}, device_id_type=MESH,
                ).wait_recv()

            pre_mate_copy().start()

        @pl.when(owner_core != core)
        def _():
            pre_mate_copy().wait_recv()

        @pl.loop(0, n)
        def _(b):
            pre = pre_all[b].astype(F32)
            slope_all[b] = silu_slope(pre)
            hid_all[b] = jax.nn.silu(pre).astype(BF16)

    def down_copy():
        return pltpu.make_async_remote_copy(
            src_ref=gin_ref, dst_ref=inc, send_sem=down_send.at[0],
            recv_sem=down_recv.at[0], device_id={"section": sec - 2}, device_id_type=MESH,
        )

    @pl.when(jnp.logical_not(is_first))
    def _():
        take_pre()
        up.relay()
        xs.begin()
        xs.relay()
        pltpu.make_async_remote_copy(
            src_ref=gin_ref, dst_ref=inc, send_sem=down_send.at[0],
            recv_sem=down_recv.at[0], device_id={"section": sec + 2}, device_id_type=MESH,
        ).wait_recv()
        make_slot_grad()
        sg.begin()

    def part_copy(b):
        return pltpu.make_async_remote_copy(
            src_ref=part_mine.at[b], dst_ref=part_other.at[b], send_sem=part_send.at[b],
            recv_sem=part_recv.at[b], device_id={"section": twin}, device_id_type=MESH,
        )

    def part_of(b):
        part_mine[b] = lax.dot_general(sg_all[b], down_ref[...], NT, preferred_element_type=F32)
        part_copy(b).start()

    def pg_copy(b):
        return pltpu.make_async_remote_copy(
            src_ref=pg_all.at[b], dst_ref=pg_own.at[me], send_sem=pg_send.at[b],
            recv_sem=pg_recv.at[me], device_id={"dp": b}, device_id_type=MESH,
        )

    def finish_of(b):
        part_copy(b).wait_recv()
        pg_all[b] = ((part_mine[b] + part_other[b]) * slope_all[b]).astype(BF16)

        @pl.when(b == me)
        def _():
            pg_own[me] = pg_all[me]

        @pl.when(b != me)
        def _():
            pg_copy(b).start()

    def add_down(b):
        gdown_ref[...] += lax.dot_general(hid_all[b], sg_all[b], TN, preferred_element_type=F32)

    def add_up(b):
        gup_ref[...] += lax.dot_general(pg_all[b], xs_all[b], TN, preferred_element_type=F32)

    def finish_row(b):
        finish_of(b)
        add_down(b)

        @pl.when(jnp.logical_not(is_first))
        def _():
            add_up(b)

    def finish_other(b):
        part_of(b)
        add_down(b)
        finish_of(b)
        xs.wait_block(b)
        add_up(b)

    part_of(me)

    @pl.when(jnp.logical_not(is_first))
    def _():
        sg.relay(part_of)

    def both_parts(b):
        part_of(b)
        part2_of(b // 2)

    @pl.when(is_first)
    def _():
        take_pre()

        @pl.loop(0, half_n)
        def _(i):
            pm_copy(i).start()

        dm_copy().wait_recv()
        part2_of(sg.at)
        sg.relay(both_parts, forward=False)
        up.begin()
        finish2(sg.at)
        sg.each_row(lambda b: finish2(b // 2))

    finish_row(me)
    sg.each_row(finish_row)

    @pl.when(jnp.logical_not(is_first))
    def _():
        sg.each_other(finish_other)

    @pl.when(is_first)
    def _():
        up.relay()

    def wait_pg(b):
        pltpu.make_async_remote_copy(
            src_ref=pg_all.at[b], dst_ref=pg_own.at[b], send_sem=pg_send.at[b],
            recv_sem=pg_recv.at[b], device_id={"dp": b}, device_id_type=MESH,
        ).wait_recv()

    acc[...] = jnp.dot(pg_own[me], up_all[me], preferred_element_type=F32)

    def add_acc(b):
        @pl.when(jnp.logical_not(jnp.logical_and(is_first, b == mate)))
        def _():
            wait_pg(b)

        acc[...] += jnp.dot(pg_own[b], up_all[b], preferred_element_type=F32)

    up.each_row(add_acc)
    up.each_other(add_acc)

    onehot_t = (slot_col[...] == lax.broadcasted_iota(jnp.int32, (slots, slots), 1)).astype(BF16)
    delta = jnp.dot(onehot_t, acc[...].astype(BF16), preferred_element_type=F32)
    gin_ref[...] = (inc[...].astype(F32) + delta).astype(BF16)

    @pl.when(pair > 0)
    def _():
        down_copy().start()

    @pl.when(is_first)
    def _():
        xs.begin()
        sg.each_row(lambda b: sg.to_mate(b // 2).start())
        xs.relay()
        add_up(me)
        xs.each_row(add_up)
        sg.each_other(add_down)

        def add_up_other(b):
            pgx_copy(b // 2, b).wait_recv()
            add_up(b)

        xs.each_other(add_up_other)

    sg.drain()
    up.drain()
    xs.drain()

    @pl.loop(0, half_n)
    def _(j):
        @pl.when(core * half_n + j != me)
        def _():
            pre_copy(j).wait_send()

    @pl.when(owner_core == core)
    def _():
        pre_mate_copy().wait_send()

    def drain_parts(b):
        part_copy(b).wait_send()

        @pl.when(b != me)
        def _():
            pg_copy(b).wait_send()

    @pl.loop(0, half_n)
    def _(i):
        drain_parts(sg.row(i))

        @pl.when(jnp.logical_not(is_first))
        def _():
            drain_parts(sg.other(i))

        @pl.when(is_first)
        def _():
            pm_copy(i).wait_send()
            p2_copy(i).wait_send()
            pgx_copy(i, sg.row(i)).wait_send()

            @pl.when(i != sg.at)
            def _():
                pg2_copy(i).wait_send()

    @pl.when(is_first)
    def _():
        dm_copy().wait_send()

    @pl.when(pair > 0)
    def _():
        down_copy().wait_send()


def local(n, layers, slot_of_token, gate_prob, layer_input, preact, top_grad, w_up, w_down):
    pair = lax.axis_index("section") // 2
    slots, half = layer_input.shape[1:]
    units = w_up.shape[0]
    slot_here = lax.dynamic_index_in_dim(slot_of_token, pair, 0, keepdims=False)
    gate_here = lax.dynamic_index_in_dim(gate_prob, pair, 0, keepdims=False)
    pre = preact[0].reshape(slots, n // 2, units).transpose(1, 0, 2)
    vmem = pl.BlockSpec(memory_space=pltpu.VMEM)
    dma = lambda count: pltpu.SemaphoreType.DMA((count,))
    wide = pltpu.VMEM((n, slots, half), BF16)
    thin = lambda dtype: pltpu.VMEM((n, slots, units), dtype)
    thin2 = lambda dtype: pltpu.VMEM((n // 2, slots, units), dtype)
    gin, gup, gdown = pl.pallas_call(
        functools.partial(kernel, n, layers),
        out_shape=[
            jax.ShapeDtypeStruct((slots, half), BF16),
            jax.ShapeDtypeStruct((units, half), F32),
            jax.ShapeDtypeStruct((units, half), F32),
        ],
        in_specs=[vmem] * 8,
        out_specs=[vmem] * 3,
        scratch_shapes=[
            wide, pltpu.VMEM((n, units, half), BF16), wide,
            thin(BF16), thin(F32), thin(BF16), thin(F32), thin(F32), thin(BF16), thin(BF16),
            pltpu.VMEM((slots, half), F32),
            pltpu.VMEM((slots, half), BF16),
            pltpu.VMEM((units, half), BF16), thin2(BF16), thin2(F32), thin2(F32), thin2(BF16),
            *([dma(n // 2), dma(n // 2), dma(n // 2), dma(n)] * 3),
            dma(n // 2), dma(n), dma(1), dma(1), dma(n), dma(n), dma(n), dma(n),
            dma(1), dma(1), dma(1), dma(1), *([dma(n // 2)] * 7),
        ],
        compiler_params=pltpu.CompilerParams(
            collective_id=0, has_side_effects=True, vmem_limit_bytes=62 * 1024 * 1024
        ),
    )(
        slot_here, slot_here.reshape(slots, 1), gate_here.reshape(slots, 1),
        layer_input[0], pre, top_grad[0], w_up, w_down,
    )
    return gin[None], gup, gdown


def solution(mesh):
    n, sections = mesh.shape["dp"], mesh.shape["section"]
    in_specs = (
        P(None, None, "dp"),
        P(None, None, "dp"),
        P(None, "dp", "section"),
        P(None, "dp", "section"),
        P(None, "dp", None),
        P("dp", "section"),
        P("dp", "section"),
    )
    out_specs = (P(None, "dp", "section"), P("dp", "section"), P("dp", "section"))
    return jax.shard_map(
        functools.partial(local, n, sections // 2), mesh=mesh, in_specs=in_specs, out_specs=out_specs, check_vma=False
    )
```

```python
import functools

import jax
import jax.numpy as jnp
from jax import lax
from jax.experimental import pallas as pl
from jax.experimental.pallas import tpu as pltpu
from jax.sharding import PartitionSpec as P

MESH = pl.DeviceIdType.MESH
BF16 = jnp.bfloat16
F32 = jnp.float32
NT = (((1,), (1,)), ((), ()))
TN = (((0,), (0,)), ((), ()))


def silu_slope(pre):
    sigmoid_val = jax.nn.sigmoid(pre)
    return sigmoid_val * (1.0 + pre * (1.0 - sigmoid_val))


class Gather:
    def __init__(self, buf, right_sem, left_sem, mate_sem, recv_sem, me, n):
        self.buf, self.recv_sem = buf, recv_sem
        self.right_sem, self.left_sem, self.mate_sem = right_sem, left_sem, mate_sem
        self.me, self.last, self.at, self.side = me, n // 2 - 1, me // 2, lax.rem(me, 2)
        self.mate = me + 1 - 2 * self.side

    def copy(self, block, to, sem):
        return pltpu.make_async_remote_copy(
            src_ref=self.buf.at[block], dst_ref=self.buf.at[block], send_sem=sem,
            recv_sem=self.recv_sem.at[block], device_id={"dp": to}, device_id_type=MESH,
        )

    def row(self, i):
        return 2 * i + self.side

    def other(self, i):
        return 2 * i + 1 - self.side

    def right(self, i):
        return self.copy(self.row(i), self.me + 2, self.right_sem.at[i])

    def left(self, i):
        return self.copy(self.row(i), self.me - 2, self.left_sem.at[i])

    def to_mate(self, i):
        return self.copy(self.row(i), self.mate, self.mate_sem.at[i])

    def go_right(self, i):
        @pl.when(self.at < self.last)
        def _():
            self.right(i).start()

    def go_left(self, i):
        @pl.when(self.at > 0)
        def _():
            self.left(i).start()

    def begin(self):
        self.go_right(self.at)
        self.go_left(self.at)
        self.to_mate(self.at).start()

    def wait_block(self, block):
        self.copy(block, self.mate, self.mate_sem.at[0]).wait_recv()

    def walk(self, visit_low, visit_high):
        @pl.loop(1, self.last + 1)
        def _(j):
            @pl.when(self.at - j >= 0)
            def _():
                visit_low(self.at - j)

            @pl.when(self.at + j <= self.last)
            def _():
                visit_high(self.at + j)

    def relay(self, use=lambda block: None, forward=True):
        def low(i):
            self.wait_block(self.row(i))
            self.go_right(i)
            if forward:
                self.to_mate(i).start()
            use(self.row(i))

        def high(i):
            self.wait_block(self.row(i))
            self.go_left(i)
            if forward:
                self.to_mate(i).start()
            use(self.row(i))

        self.walk(low, high)

    def each_row(self, use):
        self.walk(lambda i: use(self.row(i)), lambda i: use(self.row(i)))

    def each_other(self, use):
        def visit(i):
            self.wait_block(self.other(i))
            use(self.other(i))

        visit(self.at)
        self.walk(visit, visit)

    def drain(self):
        @pl.loop(0, self.last + 1)
        def _(i):
            self.to_mate(i).wait_send()

            @pl.when(jnp.logical_and(self.at < self.last, i <= self.at))
            def _():
                self.right(i).wait_send()

            @pl.when(jnp.logical_and(self.at > 0, i >= self.at))
            def _():
                self.left(i).wait_send()


def kernel(
    n, layers, slot_row, slot_col, gate_col, x_ref, pre_ref, top_ref, up_ref, down_ref,
    gin_ref, gup_ref, gdown_ref,
    sg_all, up_all, xs_all, pre_all, slope_all, hid_all, part_mine, part_other, pg_all, pg_own, acc, inc,
    down_mate, pre_m, part2_mine, part2_other, pg_m,
    sg_right, sg_left, sg_mate, sg_recv, up_right, up_left, up_mate, up_recv, xs_right, xs_left, xs_mate, xs_recv,
    pre_send, pre_recv, pre_mate_send, pre_mate_recv, part_send, part_recv, pg_send, pg_recv,
    down_send, down_recv, dm_send, dm_recv, pm_send, pm_recv, p2_send, p2_recv, pgx_send, pgx_recv, pg2_send,
):
    me = lax.axis_index("dp")
    sec = lax.axis_index("section")
    pair, core = sec // 2, lax.rem(sec, 2)
    twin = sec + 1 - 2 * core
    half_n = n // 2
    slots, half = x_ref.shape
    is_first = pair == layers - 1

    sg = Gather(sg_all, sg_right, sg_left, sg_mate, sg_recv, me, n)
    up = Gather(up_all, up_right, up_left, up_mate, up_recv, me, n)
    xs = Gather(xs_all, xs_right, xs_left, xs_mate, xs_recv, me, n)

    barrier = pltpu.get_barrier_semaphore()

    @pl.loop(1, n)
    def _(k):
        pl.semaphore_signal(barrier, inc=1, device_id={"dp": lax.rem(me + k, n)}, device_id_type=MESH)

    pl.semaphore_signal(barrier, inc=1, device_id={"section": twin}, device_id_type=MESH)

    @pl.when(pair > 0)
    def _():
        pl.semaphore_signal(barrier, inc=1, device_id={"section": sec - 2}, device_id_type=MESH)

    @pl.when(pair < layers - 1)
    def _():
        pl.semaphore_signal(barrier, inc=1, device_id={"section": sec + 2}, device_id_type=MESH)

    onehot = (slot_row[...] == lax.broadcasted_iota(jnp.int32, (slots, slots), 0)).astype(BF16)

    def make_slot_grad():
        scaled = (gate_col[...] * inc[...].astype(F32)).astype(BF16)
        sg_all[me] = jnp.dot(onehot, scaled, preferred_element_type=F32).astype(BF16)

    @pl.when(is_first)
    def _():
        inc[...] = top_ref[:, pl.ds(pl.multiple_of(core * half, 128), half)]
        make_slot_grad()

    up_all[me] = up_ref[...]

    near_pairs = (pair > 0).astype(jnp.int32) + (pair < layers - 1).astype(jnp.int32)
    pl.semaphore_wait(barrier, n + near_pairs)

    mate = sg.mate

    def dm_copy():
        return pltpu.make_async_remote_copy(
            src_ref=down_ref, dst_ref=down_mate, send_sem=dm_send.at[0],
            recv_sem=dm_recv.at[0], device_id={"dp": mate}, device_id_type=MESH,
        )

    def pm_copy(i):
        return pltpu.make_async_remote_copy(
            src_ref=pre_all.at[sg.other(i)], dst_ref=pre_m.at[i], send_sem=pm_send.at[i],
            recv_sem=pm_recv.at[i], device_id={"dp": mate}, device_id_type=MESH,
        )

    def p2_copy(i):
        return pltpu.make_async_remote_copy(
            src_ref=part2_mine.at[i], dst_ref=part2_other.at[i], send_sem=p2_send.at[i],
            recv_sem=p2_recv.at[i], device_id={"section": twin}, device_id_type=MESH,
        )

    def pgx_copy(i, block):
        return pltpu.make_async_remote_copy(
            src_ref=pg_m.at[i], dst_ref=pg_all.at[block], send_sem=pgx_send.at[i],
            recv_sem=pgx_recv.at[i], device_id={"dp": mate}, device_id_type=MESH,
        )

    def pg2_copy(i):
        return pltpu.make_async_remote_copy(
            src_ref=pg_m.at[i], dst_ref=pg_own.at[mate], send_sem=pg2_send.at[i],
            recv_sem=pg_recv.at[mate], device_id={"dp": sg.row(i)}, device_id_type=MESH,
        )

    def part2_of(i):
        part2_mine[i] = lax.dot_general(sg_all[sg.row(i)], down_mate[...], NT, preferred_element_type=F32)
        p2_copy(i).start()

    def finish2(i):
        p2_copy(i).wait_recv()
        pm_copy(i).wait_recv()
        slope = silu_slope(pre_m[i].astype(F32))
        pg_m[i] = ((part2_mine[i] + part2_other[i]) * slope).astype(BF16)
        pgx_copy(i, sg.row(i)).start()

        @pl.when(i == sg.at)
        def _():
            pg_own[mate] = pg_m[i]

        @pl.when(i != sg.at)
        def _():
            pg2_copy(i).start()

    owner_core = me // half_n

    def pre_copy(j):
        to = core * half_n + j
        return pltpu.make_async_remote_copy(
            src_ref=pre_ref.at[j], dst_ref=pre_all.at[me], send_sem=pre_send.at[j],
            recv_sem=pre_recv.at[me], device_id={"dp": to}, device_id_type=MESH,
        )

    def pre_mate_copy():
        return pltpu.make_async_remote_copy(
            src_ref=pre_all, dst_ref=pre_all, send_sem=pre_mate_send.at[0],
            recv_sem=pre_mate_recv.at[0], device_id={"section": twin}, device_id_type=MESH,
        )

    @pl.when(owner_core == core)
    def _():
        pre_all[me] = pre_ref[me - core * half_n]

    @pl.loop(0, half_n)
    def _(j):
        @pl.when(core * half_n + j != me)
        def _():
            pre_copy(j).start()

    @pl.when(is_first)
    def _():
        dm_copy().start()
        sg.begin()

    @pl.when(jnp.logical_not(is_first))
    def _():
        up.begin()

    xs_all[me] = jnp.dot(onehot, x_ref[...], preferred_element_type=F32).astype(BF16)
    gup_ref[...] = jnp.zeros_like(gup_ref)
    gdown_ref[...] = jnp.zeros_like(gdown_ref)

    def take_pre():
        @pl.when(owner_core == core)
        def _():
            @pl.loop(1, n)
            def _(k):
                src = lax.rem(me + k, n)
                pltpu.make_async_remote_copy(
                    src_ref=pre_ref.at[0], dst_ref=pre_all.at[src], send_sem=pre_send.at[0],
                    recv_sem=pre_recv.at[src], device_id={"dp": src}, device_id_type=MESH,
                ).wait_recv()

            pre_mate_copy().start()

        @pl.when(owner_core != core)
        def _():
            pre_mate_copy().wait_recv()

        @pl.loop(0, n)
        def _(b):
            pre = pre_all[b].astype(F32)
            slope_all[b] = silu_slope(pre)
            hid_all[b] = jax.nn.silu(pre).astype(BF16)

    def down_copy():
        return pltpu.make_async_remote_copy(
            src_ref=gin_ref, dst_ref=inc, send_sem=down_send.at[0],
            recv_sem=down_recv.at[0], device_id={"section": sec - 2}, device_id_type=MESH,
        )

    @pl.when(jnp.logical_not(is_first))
    def _():
        take_pre()
        up.relay()
        xs.begin()
        xs.relay()
        pltpu.make_async_remote_copy(
            src_ref=gin_ref, dst_ref=inc, send_sem=down_send.at[0],
            recv_sem=down_recv.at[0], device_id={"section": sec + 2}, device_id_type=MESH,
        ).wait_recv()
        make_slot_grad()
        sg.begin()

    def part_copy(b):
        return pltpu.make_async_remote_copy(
            src_ref=part_mine.at[b], dst_ref=part_other.at[b], send_sem=part_send.at[b],
            recv_sem=part_recv.at[b], device_id={"section": twin}, device_id_type=MESH,
        )

    def part_of(b):
        part_mine[b] = lax.dot_general(sg_all[b], down_ref[...], NT, preferred_element_type=F32)
        part_copy(b).start()

    def pg_copy(b):
        return pltpu.make_async_remote_copy(
            src_ref=pg_all.at[b], dst_ref=pg_own.at[me], send_sem=pg_send.at[b],
            recv_sem=pg_recv.at[me], device_id={"dp": b}, device_id_type=MESH,
        )

    def finish_of(b):
        part_copy(b).wait_recv()
        pg_all[b] = ((part_mine[b] + part_other[b]) * slope_all[b]).astype(BF16)

        @pl.when(b == me)
        def _():
            pg_own[me] = pg_all[me]

        @pl.when(b != me)
        def _():
            pg_copy(b).start()

    def add_down(b):
        gdown_ref[...] += lax.dot_general(hid_all[b], sg_all[b], TN, preferred_element_type=F32)

    def add_up(b):
        gup_ref[...] += lax.dot_general(pg_all[b], xs_all[b], TN, preferred_element_type=F32)

    def finish_row(b):
        finish_of(b)
        add_down(b)

        @pl.when(jnp.logical_not(is_first))
        def _():
            add_up(b)

    def finish_other(b):
        part_of(b)
        add_down(b)
        finish_of(b)
        xs.wait_block(b)
        add_up(b)

    part_of(me)

    @pl.when(jnp.logical_not(is_first))
    def _():
        sg.relay(part_of)

    @pl.when(is_first)
    def _():
        sg.relay(part_of, forward=False)
        take_pre()

        @pl.loop(0, half_n)
        def _(i):
            pm_copy(i).start()

        up.begin()
        dm_copy().wait_recv()

        @pl.loop(0, half_n)
        def _(i):
            part2_of(i)

        @pl.loop(0, half_n)
        def _(i):
            finish2(i)

    finish_row(me)
    sg.each_row(finish_row)

    @pl.when(jnp.logical_not(is_first))
    def _():
        sg.each_other(finish_other)

    @pl.when(is_first)
    def _():
        up.relay()

    def wait_pg(b):
        pltpu.make_async_remote_copy(
            src_ref=pg_all.at[b], dst_ref=pg_own.at[b], send_sem=pg_send.at[b],
            recv_sem=pg_recv.at[b], device_id={"dp": b}, device_id_type=MESH,
        ).wait_recv()

    acc[...] = jnp.dot(pg_own[me], up_all[me], preferred_element_type=F32)

    def add_acc(b):
        @pl.when(jnp.logical_not(jnp.logical_and(is_first, b == mate)))
        def _():
            wait_pg(b)

        acc[...] += jnp.dot(pg_own[b], up_all[b], preferred_element_type=F32)

    up.each_row(add_acc)
    up.each_other(add_acc)

    onehot_t = (slot_col[...] == lax.broadcasted_iota(jnp.int32, (slots, slots), 1)).astype(BF16)
    delta = jnp.dot(onehot_t, acc[...].astype(BF16), preferred_element_type=F32)
    gin_ref[...] = (inc[...].astype(F32) + delta).astype(BF16)

    @pl.when(pair > 0)
    def _():
        down_copy().start()

    @pl.when(is_first)
    def _():
        xs.begin()
        sg.each_row(lambda b: sg.to_mate(b // 2).start())
        xs.relay()
        add_up(me)
        xs.each_row(add_up)
        sg.each_other(add_down)

        def add_up_other(b):
            pgx_copy(b // 2, b).wait_recv()
            add_up(b)

        xs.each_other(add_up_other)

    sg.drain()
    up.drain()
    xs.drain()

    @pl.loop(0, half_n)
    def _(j):
        @pl.when(core * half_n + j != me)
        def _():
            pre_copy(j).wait_send()

    @pl.when(owner_core == core)
    def _():
        pre_mate_copy().wait_send()

    def drain_parts(b):
        part_copy(b).wait_send()

        @pl.when(b != me)
        def _():
            pg_copy(b).wait_send()

    @pl.loop(0, half_n)
    def _(i):
        drain_parts(sg.row(i))

        @pl.when(jnp.logical_not(is_first))
        def _():
            drain_parts(sg.other(i))

        @pl.when(is_first)
        def _():
            pm_copy(i).wait_send()
            p2_copy(i).wait_send()
            pgx_copy(i, sg.row(i)).wait_send()

            @pl.when(i != sg.at)
            def _():
                pg2_copy(i).wait_send()

    @pl.when(is_first)
    def _():
        dm_copy().wait_send()

    @pl.when(pair > 0)
    def _():
        down_copy().wait_send()


def local(n, layers, slot_of_token, gate_prob, layer_input, preact, top_grad, w_up, w_down):
    pair = lax.axis_index("section") // 2
    slots, half = layer_input.shape[1:]
    units = w_up.shape[0]
    slot_here = lax.dynamic_index_in_dim(slot_of_token, pair, 0, keepdims=False)
    gate_here = lax.dynamic_index_in_dim(gate_prob, pair, 0, keepdims=False)
    pre = preact[0].reshape(slots, n // 2, units).transpose(1, 0, 2)
    vmem = pl.BlockSpec(memory_space=pltpu.VMEM)
    dma = lambda count: pltpu.SemaphoreType.DMA((count,))
    wide = pltpu.VMEM((n, slots, half), BF16)
    thin = lambda dtype: pltpu.VMEM((n, slots, units), dtype)
    thin2 = lambda dtype: pltpu.VMEM((n // 2, slots, units), dtype)
    gin, gup, gdown = pl.pallas_call(
        functools.partial(kernel, n, layers),
        out_shape=[
            jax.ShapeDtypeStruct((slots, half), BF16),
            jax.ShapeDtypeStruct((units, half), F32),
            jax.ShapeDtypeStruct((units, half), F32),
        ],
        in_specs=[vmem] * 8,
        out_specs=[vmem] * 3,
        scratch_shapes=[
            wide, pltpu.VMEM((n, units, half), BF16), wide,
            thin(BF16), thin(F32), thin(BF16), thin(F32), thin(F32), thin(BF16), thin(BF16),
            pltpu.VMEM((slots, half), F32),
            pltpu.VMEM((slots, half), BF16),
            pltpu.VMEM((units, half), BF16), thin2(BF16), thin2(F32), thin2(F32), thin2(BF16),
            *([dma(n // 2), dma(n // 2), dma(n // 2), dma(n)] * 3),
            dma(n // 2), dma(n), dma(1), dma(1), dma(n), dma(n), dma(n), dma(n),
            dma(1), dma(1), dma(1), dma(1), *([dma(n // 2)] * 7),
        ],
        compiler_params=pltpu.CompilerParams(
            collective_id=0, has_side_effects=True, vmem_limit_bytes=62 * 1024 * 1024
        ),
    )(
        slot_here, slot_here.reshape(slots, 1), gate_here.reshape(slots, 1),
        layer_input[0], pre, top_grad[0], w_up, w_down,
    )
    return gin[None], gup, gdown


def solution(mesh):
    n, sections = mesh.shape["dp"], mesh.shape["section"]
    in_specs = (
        P(None, None, "dp"),
        P(None, None, "dp"),
        P(None, "dp", "section"),
        P(None, "dp", "section"),
        P(None, "dp", None),
        P("dp", "section"),
        P("dp", "section"),
    )
    out_specs = (P(None, "dp", "section"), P("dp", "section"), P("dp", "section"))
    return jax.shard_map(
        functools.partial(local, n, sections // 2), mesh=mesh, in_specs=in_specs, out_specs=out_specs, check_vma=False
    )
```

```python
import functools

import jax
import jax.numpy as jnp
from jax import lax
from jax.experimental import pallas as pl
from jax.experimental.pallas import tpu as pltpu
from jax.sharding import PartitionSpec as P

MESH = pl.DeviceIdType.MESH
BF16 = jnp.bfloat16
F32 = jnp.float32
NT = (((1,), (1,)), ((), ()))
TN = (((0,), (0,)), ((), ()))


def silu_slope(pre):
    sigmoid_val = jax.nn.sigmoid(pre)
    return sigmoid_val * (1.0 + pre * (1.0 - sigmoid_val))


class Gather:
    def __init__(self, buf, right_sem, left_sem, mate_sem, recv_sem, me, n):
        self.buf, self.recv_sem = buf, recv_sem
        self.right_sem, self.left_sem, self.mate_sem = right_sem, left_sem, mate_sem
        self.me, self.last, self.at, self.side = me, n // 2 - 1, me // 2, lax.rem(me, 2)
        self.mate = me + 1 - 2 * self.side

    def copy(self, block, to, sem):
        return pltpu.make_async_remote_copy(
            src_ref=self.buf.at[block], dst_ref=self.buf.at[block], send_sem=sem,
            recv_sem=self.recv_sem.at[block], device_id={"dp": to}, device_id_type=MESH,
        )

    def row(self, i):
        return 2 * i + self.side

    def other(self, i):
        return 2 * i + 1 - self.side

    def right(self, i):
        return self.copy(self.row(i), self.me + 2, self.right_sem.at[i])

    def left(self, i):
        return self.copy(self.row(i), self.me - 2, self.left_sem.at[i])

    def to_mate(self, i):
        return self.copy(self.row(i), self.mate, self.mate_sem.at[i])

    def go_right(self, i):
        @pl.when(self.at < self.last)
        def _():
            self.right(i).start()

    def go_left(self, i):
        @pl.when(self.at > 0)
        def _():
            self.left(i).start()

    def begin(self):
        self.go_right(self.at)
        self.go_left(self.at)
        self.to_mate(self.at).start()

    def wait_block(self, block):
        self.copy(block, self.mate, self.mate_sem.at[0]).wait_recv()

    def walk(self, visit_low, visit_high):
        @pl.loop(1, self.last + 1)
        def _(j):
            @pl.when(self.at - j >= 0)
            def _():
                visit_low(self.at - j)

            @pl.when(self.at + j <= self.last)
            def _():
                visit_high(self.at + j)

    def relay(self, use=lambda block: None, forward=True):
        def low(i):
            self.wait_block(self.row(i))
            self.go_right(i)
            if forward:
                self.to_mate(i).start()
            use(self.row(i))

        def high(i):
            self.wait_block(self.row(i))
            self.go_left(i)
            if forward:
                self.to_mate(i).start()
            use(self.row(i))

        self.walk(low, high)

    def each_row(self, use):
        self.walk(lambda i: use(self.row(i)), lambda i: use(self.row(i)))

    def each_other(self, use):
        def visit(i):
            self.wait_block(self.other(i))
            use(self.other(i))

        visit(self.at)
        self.walk(visit, visit)

    def drain(self):
        @pl.loop(0, self.last + 1)
        def _(i):
            self.to_mate(i).wait_send()

            @pl.when(jnp.logical_and(self.at < self.last, i <= self.at))
            def _():
                self.right(i).wait_send()

            @pl.when(jnp.logical_and(self.at > 0, i >= self.at))
            def _():
                self.left(i).wait_send()


def kernel(
    n, layers, slot_row, slot_col, gate_col, x_ref, pre_ref, top_ref, up_ref, down_ref,
    gin_ref, gup_ref, gdown_ref,
    sg_all, up_all, xs_all, pre_all, slope_all, hid_all, part_mine, part_other, pg_all, pg_own, acc, inc,
    down_mate, pre_m, part2_mine, part2_other, pg_m,
    sg_right, sg_left, sg_mate, sg_recv, up_right, up_left, up_mate, up_recv, xs_right, xs_left, xs_mate, xs_recv,
    pre_send, pre_recv, pre_mate_send, pre_mate_recv, part_send, part_recv, pg_send, pg_recv,
    down_send, down_recv, dm_send, dm_recv, pm_send, pm_recv, p2_send, p2_recv, pgx_send, pgx_recv, pg2_send,
):
    me = lax.axis_index("dp")
    sec = lax.axis_index("section")
    pair, core = sec // 2, lax.rem(sec, 2)
    twin = sec + 1 - 2 * core
    half_n = n // 2
    slots, half = x_ref.shape
    is_first = pair == layers - 1

    sg = Gather(sg_all, sg_right, sg_left, sg_mate, sg_recv, me, n)
    up = Gather(up_all, up_right, up_left, up_mate, up_recv, me, n)
    xs = Gather(xs_all, xs_right, xs_left, xs_mate, xs_recv, me, n)

    barrier = pltpu.get_barrier_semaphore()

    @pl.loop(1, n)
    def _(k):
        pl.semaphore_signal(barrier, inc=1, device_id={"dp": lax.rem(me + k, n)}, device_id_type=MESH)

    pl.semaphore_signal(barrier, inc=1, device_id={"section": twin}, device_id_type=MESH)

    @pl.when(pair > 0)
    def _():
        pl.semaphore_signal(barrier, inc=1, device_id={"section": sec - 2}, device_id_type=MESH)

    @pl.when(pair < layers - 1)
    def _():
        pl.semaphore_signal(barrier, inc=1, device_id={"section": sec + 2}, device_id_type=MESH)

    onehot = (slot_row[...] == lax.broadcasted_iota(jnp.int32, (slots, slots), 0)).astype(BF16)

    def make_slot_grad():
        scaled = (gate_col[...] * inc[...].astype(F32)).astype(BF16)
        sg_all[me] = jnp.dot(onehot, scaled, preferred_element_type=F32).astype(BF16)

    @pl.when(is_first)
    def _():
        inc[...] = top_ref[:, pl.ds(pl.multiple_of(core * half, 128), half)]
        make_slot_grad()

    up_all[me] = up_ref[...]

    near_pairs = (pair > 0).astype(jnp.int32) + (pair < layers - 1).astype(jnp.int32)
    pl.semaphore_wait(barrier, n + near_pairs)

    mate = sg.mate

    def dm_copy():
        return pltpu.make_async_remote_copy(
            src_ref=down_ref, dst_ref=down_mate, send_sem=dm_send.at[0],
            recv_sem=dm_recv.at[0], device_id={"dp": mate}, device_id_type=MESH,
        )

    def pm_copy(i):
        return pltpu.make_async_remote_copy(
            src_ref=pre_all.at[sg.other(i)], dst_ref=pre_m.at[i], send_sem=pm_send.at[i],
            recv_sem=pm_recv.at[i], device_id={"dp": mate}, device_id_type=MESH,
        )

    def p2_copy(i):
        return pltpu.make_async_remote_copy(
            src_ref=part2_mine.at[i], dst_ref=part2_other.at[i], send_sem=p2_send.at[i],
            recv_sem=p2_recv.at[i], device_id={"section": twin}, device_id_type=MESH,
        )

    def pgx_copy(i, block):
        return pltpu.make_async_remote_copy(
            src_ref=pg_m.at[i], dst_ref=pg_all.at[block], send_sem=pgx_send.at[i],
            recv_sem=pgx_recv.at[i], device_id={"dp": mate}, device_id_type=MESH,
        )

    def pg2_copy(i):
        return pltpu.make_async_remote_copy(
            src_ref=pg_m.at[i], dst_ref=pg_own.at[mate], send_sem=pg2_send.at[i],
            recv_sem=pg_recv.at[mate], device_id={"dp": sg.row(i)}, device_id_type=MESH,
        )

    def part2_of(i):
        part2_mine[i] = lax.dot_general(sg_all[sg.row(i)], down_mate[...], NT, preferred_element_type=F32)
        p2_copy(i).start()

    def finish2(i):
        p2_copy(i).wait_recv()
        pm_copy(i).wait_recv()
        slope = silu_slope(pre_m[i].astype(F32))
        pg_m[i] = ((part2_mine[i] + part2_other[i]) * slope).astype(BF16)
        pgx_copy(i, sg.row(i)).start()

        @pl.when(i == sg.at)
        def _():
            pg_own[mate] = pg_m[i]

        @pl.when(i != sg.at)
        def _():
            pg2_copy(i).start()

    owner_core = me // half_n

    def pre_copy(j):
        to = core * half_n + j
        return pltpu.make_async_remote_copy(
            src_ref=pre_ref.at[j], dst_ref=pre_all.at[me], send_sem=pre_send.at[j],
            recv_sem=pre_recv.at[me], device_id={"dp": to}, device_id_type=MESH,
        )

    def pre_mate_copy():
        return pltpu.make_async_remote_copy(
            src_ref=pre_all, dst_ref=pre_all, send_sem=pre_mate_send.at[0],
            recv_sem=pre_mate_recv.at[0], device_id={"section": twin}, device_id_type=MESH,
        )

    @pl.when(owner_core == core)
    def _():
        pre_all[me] = pre_ref[me - core * half_n]

    @pl.loop(0, half_n)
    def _(j):
        @pl.when(core * half_n + j != me)
        def _():
            pre_copy(j).start()

    @pl.when(is_first)
    def _():
        dm_copy().start()
        sg.begin()

    @pl.when(jnp.logical_not(is_first))
    def _():
        up.begin()

    xs_all[me] = jnp.dot(onehot, x_ref[...], preferred_element_type=F32).astype(BF16)
    gup_ref[...] = jnp.zeros_like(gup_ref)
    gdown_ref[...] = jnp.zeros_like(gdown_ref)

    def take_pre():
        @pl.when(owner_core == core)
        def _():
            @pl.loop(1, n)
            def _(k):
                src = lax.rem(me + k, n)
                pltpu.make_async_remote_copy(
                    src_ref=pre_ref.at[0], dst_ref=pre_all.at[src], send_sem=pre_send.at[0],
                    recv_sem=pre_recv.at[src], device_id={"dp": src}, device_id_type=MESH,
                ).wait_recv()

            pre_mate_copy().start()

        @pl.when(owner_core != core)
        def _():
            pre_mate_copy().wait_recv()

        @pl.loop(0, n)
        def _(b):
            pre = pre_all[b].astype(F32)
            slope_all[b] = silu_slope(pre)
            hid_all[b] = jax.nn.silu(pre).astype(BF16)

    def down_copy():
        return pltpu.make_async_remote_copy(
            src_ref=gin_ref, dst_ref=inc, send_sem=down_send.at[0],
            recv_sem=down_recv.at[0], device_id={"section": sec - 2}, device_id_type=MESH,
        )

    @pl.when(jnp.logical_not(is_first))
    def _():
        take_pre()
        up.relay()
        xs.begin()
        xs.relay()
        pltpu.make_async_remote_copy(
            src_ref=gin_ref, dst_ref=inc, send_sem=down_send.at[0],
            recv_sem=down_recv.at[0], device_id={"section": sec + 2}, device_id_type=MESH,
        ).wait_recv()
        make_slot_grad()
        sg.begin()

    def part_copy(b):
        return pltpu.make_async_remote_copy(
            src_ref=part_mine.at[b], dst_ref=part_other.at[b], send_sem=part_send.at[b],
            recv_sem=part_recv.at[b], device_id={"section": twin}, device_id_type=MESH,
        )

    def part_of(b):
        part_mine[b] = lax.dot_general(sg_all[b], down_ref[...], NT, preferred_element_type=F32)
        part_copy(b).start()

    def pg_copy(b):
        return pltpu.make_async_remote_copy(
            src_ref=pg_all.at[b], dst_ref=pg_own.at[me], send_sem=pg_send.at[b],
            recv_sem=pg_recv.at[me], device_id={"dp": b}, device_id_type=MESH,
        )

    def finish_of(b):
        part_copy(b).wait_recv()
        pg_all[b] = ((part_mine[b] + part_other[b]) * slope_all[b]).astype(BF16)

        @pl.when(b == me)
        def _():
            pg_own[me] = pg_all[me]

        @pl.when(b != me)
        def _():
            pg_copy(b).start()

    def add_down(b):
        gdown_ref[...] += lax.dot_general(hid_all[b], sg_all[b], TN, preferred_element_type=F32)

    def add_up(b):
        gup_ref[...] += lax.dot_general(pg_all[b], xs_all[b], TN, preferred_element_type=F32)

    def finish_row(b):
        finish_of(b)
        add_down(b)

        @pl.when(jnp.logical_not(is_first))
        def _():
            add_up(b)

    def finish_other(b):
        part_of(b)
        add_down(b)
        finish_of(b)
        xs.wait_block(b)
        add_up(b)

    part_of(me)

    @pl.when(jnp.logical_not(is_first))
    def _():
        sg.relay(part_of)

    @pl.when(is_first)
    def _():
        sg.relay(part_of, forward=False)
        take_pre()

        @pl.loop(0, half_n)
        def _(i):
            pm_copy(i).start()

        up.begin()
        up.relay()
        dm_copy().wait_recv()

        @pl.loop(0, half_n)
        def _(i):
            part2_of(i)

        @pl.loop(0, half_n)
        def _(i):
            finish2(i)

    finish_row(me)
    sg.each_row(finish_row)

    @pl.when(jnp.logical_not(is_first))
    def _():
        sg.each_other(finish_other)


    def wait_pg(b):
        pltpu.make_async_remote_copy(
            src_ref=pg_all.at[b], dst_ref=pg_own.at[b], send_sem=pg_send.at[b],
            recv_sem=pg_recv.at[b], device_id={"dp": b}, device_id_type=MESH,
        ).wait_recv()

    acc[...] = jnp.dot(pg_own[me], up_all[me], preferred_element_type=F32)

    def add_acc(b):
        @pl.when(jnp.logical_not(jnp.logical_and(is_first, b == mate)))
        def _():
            wait_pg(b)

        acc[...] += jnp.dot(pg_own[b], up_all[b], preferred_element_type=F32)

    up.each_row(add_acc)
    up.each_other(add_acc)

    onehot_t = (slot_col[...] == lax.broadcasted_iota(jnp.int32, (slots, slots), 1)).astype(BF16)
    delta = jnp.dot(onehot_t, acc[...].astype(BF16), preferred_element_type=F32)
    gin_ref[...] = (inc[...].astype(F32) + delta).astype(BF16)

    @pl.when(pair > 0)
    def _():
        down_copy().start()

    @pl.when(is_first)
    def _():
        xs.begin()
        sg.each_row(lambda b: sg.to_mate(b // 2).start())
        xs.relay()
        add_up(me)
        xs.each_row(add_up)
        sg.each_other(add_down)

        def add_up_other(b):
            pgx_copy(b // 2, b).wait_recv()
            add_up(b)

        xs.each_other(add_up_other)

    sg.drain()
    up.drain()
    xs.drain()

    @pl.loop(0, half_n)
    def _(j):
        @pl.when(core * half_n + j != me)
        def _():
            pre_copy(j).wait_send()

    @pl.when(owner_core == core)
    def _():
        pre_mate_copy().wait_send()

    def drain_parts(b):
        part_copy(b).wait_send()

        @pl.when(b != me)
        def _():
            pg_copy(b).wait_send()

    @pl.loop(0, half_n)
    def _(i):
        drain_parts(sg.row(i))

        @pl.when(jnp.logical_not(is_first))
        def _():
            drain_parts(sg.other(i))

        @pl.when(is_first)
        def _():
            pm_copy(i).wait_send()
            p2_copy(i).wait_send()
            pgx_copy(i, sg.row(i)).wait_send()

            @pl.when(i != sg.at)
            def _():
                pg2_copy(i).wait_send()

    @pl.when(is_first)
    def _():
        dm_copy().wait_send()

    @pl.when(pair > 0)
    def _():
        down_copy().wait_send()


def local(n, layers, slot_of_token, gate_prob, layer_input, preact, top_grad, w_up, w_down):
    pair = lax.axis_index("section") // 2
    slots, half = layer_input.shape[1:]
    units = w_up.shape[0]
    slot_here = lax.dynamic_index_in_dim(slot_of_token, pair, 0, keepdims=False)
    gate_here = lax.dynamic_index_in_dim(gate_prob, pair, 0, keepdims=False)
    pre = preact[0].reshape(slots, n // 2, units).transpose(1, 0, 2)
    vmem = pl.BlockSpec(memory_space=pltpu.VMEM)
    dma = lambda count: pltpu.SemaphoreType.DMA((count,))
    wide = pltpu.VMEM((n, slots, half), BF16)
    thin = lambda dtype: pltpu.VMEM((n, slots, units), dtype)
    thin2 = lambda dtype: pltpu.VMEM((n // 2, slots, units), dtype)
    gin, gup, gdown = pl.pallas_call(
        functools.partial(kernel, n, layers),
        out_shape=[
            jax.ShapeDtypeStruct((slots, half), BF16),
            jax.ShapeDtypeStruct((units, half), F32),
            jax.ShapeDtypeStruct((units, half), F32),
        ],
        in_specs=[vmem] * 8,
        out_specs=[vmem] * 3,
        scratch_shapes=[
            wide, pltpu.VMEM((n, units, half), BF16), wide,
            thin(BF16), thin(F32), thin(BF16), thin(F32), thin(F32), thin(BF16), thin(BF16),
            pltpu.VMEM((slots, half), F32),
            pltpu.VMEM((slots, half), BF16),
            pltpu.VMEM((units, half), BF16), thin2(BF16), thin2(F32), thin2(F32), thin2(BF16),
            *([dma(n // 2), dma(n // 2), dma(n // 2), dma(n)] * 3),
            dma(n // 2), dma(n), dma(1), dma(1), dma(n), dma(n), dma(n), dma(n),
            dma(1), dma(1), dma(1), dma(1), *([dma(n // 2)] * 7),
        ],
        compiler_params=pltpu.CompilerParams(
            collective_id=0, has_side_effects=True, vmem_limit_bytes=62 * 1024 * 1024
        ),
    )(
        slot_here, slot_here.reshape(slots, 1), gate_here.reshape(slots, 1),
        layer_input[0], pre, top_grad[0], w_up, w_down,
    )
    return gin[None], gup, gdown


def solution(mesh):
    n, sections = mesh.shape["dp"], mesh.shape["section"]
    in_specs = (
        P(None, None, "dp"),
        P(None, None, "dp"),
        P(None, "dp", "section"),
        P(None, "dp", "section"),
        P(None, "dp", None),
        P("dp", "section"),
        P("dp", "section"),
    )
    out_specs = (P(None, "dp", "section"), P("dp", "section"), P("dp", "section"))
    return jax.shard_map(
        functools.partial(local, n, sections // 2), mesh=mesh, in_specs=in_specs, out_specs=out_specs, check_vma=False
    )
```
